32 devices in a mesh: gx: 8 (over z, y), gy: 4 (over x, core).
Axes of the slice: x: 2, y: 2, z: 4, core: 2. Of those that a mesh axis runs over, the one named last changes fastest.
Arguments:
- right_side: float32 [64, 128, 128], P('gy', 'gx'), may hold values from -6 to 9
- diagonal: float32 [64, 128, 128], P('gy', 'gx'), may hold values from 0.02 to 0.5
- horizontal: float32 [64, 128, 128], P('gy', 'gx'), may hold values from 0.1 to 1
- vertical: float32 [128], replicated, may hold values from 0.2 to 2
- precond: float32 [2, 128, 128], replicated, may hold values from -4 to 4
- edge_rows: int32 [2, 64], replicated, may hold values from 0 to 63, as said below
Outputs:
- solution_field: float32 [64, 128, 128], P('gy', 'gx')
- residual: float32 [64, 128, 128], P('gy', 'gx')
- residual_sq: float32 [3], replicated
The draws below stay inside these ranges and needn't reach their ends.
Inputs may be any that keep to these rules, and one draw needn't show every extreme that they name: Each row of edge_rows lists every number 0 to 63 exactly once.
All inputs are finite; a program needn't handle non-finite values.
Results may differ from the reference program's by a relative error of at most 0.00014.
Values sent between devices are 32-bit elements; how exact they have to be, the bound alone decides.
A program may use at most 64 MiB of HBM per device.

```python
import math
import jax
import jax.numpy as jnp
from jax import lax

LEV = 128
ITERS = 3
NX = 128
NY = 64


def draw_right_side(key, part):
    base = jnp.clip(jax.random.normal(key, (NY, NX, LEV), jnp.float32), -6.0, 6.0)
    return base


def draw_precond(key, part):
    keys = jax.random.split(key, 3)
    extra = jax.random.uniform(keys[0], (2, LEV), jnp.float32, 0.3, 1.0)
    couple = jax.random.uniform(keys[1], (2, LEV - 1), jnp.float32, 0.5, 2.0)
    padded = jnp.pad(couple, ((0, 0), (1, 1)))
    main = extra + padded[:, :-1] + padded[:, 1:]
    couple_row = jnp.pad(couple, ((0, 0), (0, 1)))
    upper = jnp.eye(LEV, k=1, dtype=jnp.float32)
    lower = jnp.eye(LEV, k=-1, dtype=jnp.float32)
    eye = jnp.eye(LEV, dtype=jnp.float32)
    tri = main[:, :, None] * eye[None] - couple_row[:, :, None] * upper[None] - couple_row[:, None, :] * lower[None]
    inverse = jnp.linalg.inv(tri)
    size = jnp.mean(jnp.abs(jnp.diagonal(inverse, axis1=1, axis2=2)), axis=1)
    noise = jax.random.normal(keys[2], (2, LEV, LEV), jnp.float32)
    return inverse + 0.05 * size[:, None, None] * noise


def draw_edge_rows(key, part):
    first = jax.random.permutation(jax.random.fold_in(key, 11), NY).astype(jnp.int32)
    second = jax.random.permutation(jax.random.fold_in(key, 23), NY).astype(jnp.int32)
    return jnp.stack([first, second]).astype(jnp.int32)


def block_scale(rng, dims, pieces, least, largest):
    loudness = 1.0
    for dim, parts in pieces:
        draws = jax.random.uniform(jax.random.fold_in(jax.random.fold_in(rng, 6), dim), (parts,), jnp.float32, least / len(pieces), largest / len(pieces))
        loudness = loudness * jnp.repeat(jnp.exp(draws), dims[dim] // parts).reshape((-1,) + (1,) * (len(dims) - 1 - dim))
    return loudness


def setup_inputs(seed: int = 0) -> dict:
    seeds = jax.random.split(jax.random.key(seed), 7)
    right_side = draw_right_side(jax.random.fold_in(seeds[6], 71), 0)
    diagonal = jnp.clip(jnp.exp(math.log(0.5) - 3.218876 * jax.random.uniform(seeds[1], (NY, NX, LEV), jnp.float32) ** block_scale(seeds[1], (NY, NX, LEV), ((0, 4), (1, 8)), -0.2, 0.2)), 0.02, 0.5)
    horizontal = jnp.clip(jnp.exp(math.log(1.0) - 2.3025851 * jax.random.uniform(seeds[2], (NY, NX, LEV), jnp.float32) ** block_scale(seeds[2], (NY, NX, LEV), ((0, 4), (1, 8)), -0.2, 0.2)), 0.1, 1.0)
    vertical = jnp.clip(jnp.exp(jax.random.uniform(seeds[3], (LEV,), jnp.float32, math.log(0.2), math.log(2.0))), 0.2, 2.0)
    precond = draw_precond(jax.random.fold_in(seeds[6], 71), 0)
    edge_rows = draw_edge_rows(jax.random.fold_in(seeds[6], 71), 0)
    return dict(right_side=right_side, diagonal=diagonal, horizontal=horizontal, vertical=vertical, precond=precond, edge_rows=edge_rows)


def operate(field, diagonal, horizontal, vertical, edge_rows):
    width = field.shape[1]
    half = width // 2
    east = jnp.roll(field, -1, 1)
    east = east.at[:, half - 1].set(field[edge_rows[0], half]).at[:, width - 1].set(field[edge_rows[1], 0])
    west = jnp.roll(field, 1, 1)
    west = west.at[:, half].set(field[edge_rows[0], half - 1]).at[:, 0].set(field[edge_rows[1], width - 1])
    tall = jnp.pad(field, ((1, 1), (0, 0), (0, 0)))
    flat = jnp.pad(field, ((0, 0), (0, 0), (1, 1)))
    beside = east + west + tall[2:] + tall[:-2]
    column = flat[:, :, 2:] + flat[:, :, :-2]
    return diagonal * field + horizontal * (4.0 * field - beside) + vertical * (2.0 * field - column)

def precondition(field, precond):
    half = field.shape[1] // 2
    left = jnp.einsum('yxl,kl->yxk', field[:, :half], precond[0], precision=lax.Precision.HIGHEST)
    right = jnp.einsum('yxl,kl->yxk', field[:, half:], precond[1], precision=lax.Precision.HIGHEST)
    return jnp.concatenate([left, right], 1)

def reference(right_side, diagonal, horizontal, vertical, precond, edge_rows):
    total_cells = float(right_side.size)

    def inner(left, right):
        return jnp.sum(left * right) / total_cells
    solution_field = jnp.zeros_like(right_side)
    residual = right_side
    directions = []
    images = []
    norms = []
    for step in range(ITERS):
        pre = precondition(residual, precond)
        image = operate(pre, diagonal, horizontal, vertical, edge_rows)
        coeffs = [inner(image, older) for older in images]
        for number in range(len(images)):
            pre = pre - coeffs[number] * directions[number]
            image = image - coeffs[number] * images[number]
        scale = 1.0 / jnp.sqrt(inner(image, image))
        direction = pre * scale
        image = image * scale
        alpha = inner(residual, image)
        solution_field = solution_field + alpha * direction
        residual = residual - alpha * image
        norms.append(inner(residual, residual))
        directions.append(direction)
        images.append(image)
    return (solution_field, residual, jnp.stack(norms))
```

```python
import functools

import jax
import jax.numpy as jnp
from jax import lax
from jax.experimental import pallas as pl
from jax.experimental.pallas import tpu as pltpu
from jax.sharding import PartitionSpec as P

ITERS = 3
MESH = pl.DeviceIdType.MESH
ANY = pl.BlockSpec(memory_space=pl.ANY)
VMEM = pl.BlockSpec(memory_space=pltpu.VMEM)
SMEM = pl.BlockSpec(memory_space=pltpu.SMEM)


def kernel(
    n_gx,
    n_gy,
    edge_rows,
    right_side,
    diagonal,
    horizontal,
    vertical,
    precond,
    out_x,
    out_r,
    out_norms,
    r0,
    diag,
    horiz,
    vert,
    matrix,
    fields,
    images,
    send_cols,
    from_east,
    from_west,
    from_north,
    from_south,
    east_col,
    west_col,
    sums,
    load_sem,
    col_send,
    east_recv,
    west_recv,
    row_send,
    north_recv,
    south_recv,
    sum_send,
    sum_recv,
):
    rows, cols, levels = r0.shape
    gx, gy = lax.axis_index("gx"), lax.axis_index("gy")
    n_all = n_gx * n_gy
    half = n_gx // 2
    me = gx * n_gy + gy
    total_cells = float(rows * cols * levels * n_all)

    def for_others(visit):
        for j in range(1, n_gy):
            visit(gx, lax.rem(gy + j, n_gy))

        def step(i, carry):
            for j in range(n_gy):
                visit(lax.rem(gx + i, n_gx), lax.rem(gy + j, n_gy))
            return carry

        if n_all <= 64:
            for i in range(1, n_gx):
                step(i, 0)
        else:
            lax.fori_loop(1, n_gx, step, 0)

    barrier = pltpu.get_barrier_semaphore()

    def greet(x, y):
        pl.semaphore_signal(barrier, inc=1, device_id=(x, y), device_id_type=MESH)

    for_others(greet)

    panel = lax.convert_element_type(gx >= half, jnp.int32)
    loads = [
        pltpu.make_async_copy(right_side, r0, load_sem.at[0]),
        pltpu.make_async_copy(precond.at[panel], matrix, load_sem.at[1]),
        pltpu.make_async_copy(diagonal, diag, load_sem.at[2]),
        pltpu.make_async_copy(horizontal, horiz, load_sem.at[3]),
        pltpu.make_async_copy(vertical, vert, load_sem.at[4]),
    ]
    for load in loads:
        load.start()

    east_x, west_x = lax.rem(gx + 1, n_gx), lax.rem(gx + n_gx - 1, n_gx)
    east_border = (gx == half - 1) | (gx == n_gx - 1)
    west_border = (gx == half) | (gx == 0)
    east_table = jnp.where(gx == half - 1, 0, 1)
    west_table = jnp.where(gx == half, 0, 1)
    first_row = gy * rows
    has_north, has_south = gy < n_gy - 1, gy > 0

    @pl.when(jnp.logical_not(has_north))
    def _():
        from_north[...] = jnp.zeros_like(from_north)

    @pl.when(jnp.logical_not(has_south))
    def _():
        from_south[...] = jnp.zeros_like(from_south)

    def flat(v):
        return v.reshape(rows * cols, levels)

    def precondition(v):
        return lax.dot_general(
            flat(v),
            matrix[...],
            (((1,), (1,)), ((), ())),
            precision=lax.Precision.HIGHEST,
            preferred_element_type=jnp.float32,
        ).reshape(rows, cols, levels)

    def col_copy(t, side, g):
        buffer, recv, x = (
            (from_west, west_recv, east_x) if side == 0 else (from_east, east_recv, west_x)
        )
        return pltpu.make_async_remote_copy(
            src_ref=send_cols.at[t, side],
            dst_ref=buffer[t].at[pl.ds(first_row, rows)],
            send_sem=col_send.at[t, side],
            recv_sem=recv.at[t],
            device_id=(x, g),
            device_id_type=MESH,
        )

    def row_copy(t, side):
        buffer, recv, y, row = (
            (from_south, south_recv, gy + 1, rows - 1)
            if side == 0
            else (from_north, north_recv, gy - 1, 0)
        )
        return pltpu.make_async_remote_copy(
            src_ref=fields.at[t, row],
            dst_ref=buffer.at[t],
            send_sem=row_send.at[t, side],
            recv_sem=recv.at[t],
            device_id=(gx, y),
            device_id_type=MESH,
        )

    def send(t):
        for side, border in ((0, east_border), (1, west_border)):
            for g in range(n_gy):
                @pl.when(border | (gy == g))
                def _(side=side, g=g):
                    col_copy(t, side, g).start()

        @pl.when(has_north)
        def _():
            row_copy(t, 0).start()

        @pl.when(has_south)
        def _():
            row_copy(t, 1).start()

    def wait_cols(border, sem):
        whole = from_east[0]
        part = whole.at[pl.ds(0, rows)]

        @pl.when(border)
        def _():
            pltpu.make_async_copy(whole, whole, sem).wait()

        @pl.when(jnp.logical_not(border))
        def _():
            pltpu.make_async_copy(part, part, sem).wait()

    def receive(t):
        @pl.when(has_north)
        def _():
            row_copy(t, 1).wait_recv()

        @pl.when(has_south)
        def _():
            row_copy(t, 0).wait_recv()

        for border, recv, buffer, table, col in (
            (east_border, east_recv, from_east, east_table, east_col),
            (west_border, west_recv, from_west, west_table, west_col),
        ):
            wait_cols(border, recv.at[t])

            @pl.when(border)
            def _(buffer=buffer, table=table, col=col):
                for y in range(rows):
                    col[y] = buffer[t][edge_rows[table, first_row + y]]

            @pl.when(jnp.logical_not(border))
            def _(buffer=buffer, col=col):
                col[...] = buffer[t][pl.ds(first_row, rows)]

    col_id = lax.broadcasted_iota(jnp.int32, (rows, cols, levels), 1)
    lane_id = lax.broadcasted_iota(jnp.int32, (rows * cols, levels), 1)

    def local_part(z):
        flat_z = flat(z)
        up = jnp.where(lane_id < levels - 1, pltpu.roll(flat_z, levels - 1, 1), 0.0)
        down = jnp.where(lane_id > 0, pltpu.roll(flat_z, 1, 1), 0.0)
        column = (up + down).reshape(rows, cols, levels)
        v = vert[...].reshape(1, 1, levels)
        return diag[...] * z + v * (2.0 * z - column)

    def image_of(t, z, base):
        east = jnp.where(col_id == cols - 1, east_col[...], pltpu.roll(z, cols - 1, 1))
        west = jnp.where(col_id == 0, west_col[...], pltpu.roll(z, 1, 1))
        north = jnp.concatenate([z[1:], from_north[t][None]], 0)
        south = jnp.concatenate([from_south[t][None], z[:-1]], 0)
        return base + horiz[...] * (4.0 * z - (east + west + north + south))

    def product(a, b):
        both = (a * b).reshape(rows * cols // 8, 8, levels)
        return jnp.sum(jnp.sum(both, axis=0), axis=0, keepdims=True)

    loads[0].wait()
    loads[1].wait()
    terms = {}
    spaces = [r0]
    for t in range(ITERS):
        z = precondition(spaces[-1][...])
        fields[t] = z
        send_cols[t, 0] = z[:, cols - 1 : cols, :]
        send_cols[t, 1] = z[:, 0:1, :]
        if t == 0:
            pl.semaphore_wait(barrier, n_all - 1)
        send(t)
        if t == 0:
            for load in loads[2:]:
                load.wait()
        newest = len(spaces) - 1
        for i in range(len(spaces)):
            terms[(i, newest)] = product(spaces[i][...], spaces[newest][...])
        base = local_part(z)
        receive(t)
        images[t] = image_of(t, z, base)
        spaces.append(images.at[t])
    newest = len(spaces) - 1
    for i in range(len(spaces)):
        terms[(i, newest)] = product(spaces[i][...], spaces[newest][...])

    keys = list(terms)
    height = -(-len(keys) // 8) * 8
    row_id = lax.broadcasted_iota(jnp.int32, (height, levels), 0)
    lane = lax.broadcasted_iota(jnp.int32, (height, levels), 1)
    stacked = jnp.zeros((height, levels), jnp.float32)
    for k, key in enumerate(keys):
        stacked = jnp.where(row_id == k, terms[key], stacked)
    summed = jnp.sum(stacked, axis=1, keepdims=True)
    sums[me] = jnp.sum(jnp.where(lane == row_id, summed, 0.0), axis=0, keepdims=True)

    def tell(x, y):
        pltpu.make_async_remote_copy(
            src_ref=sums.at[me],
            dst_ref=sums.at[me],
            send_sem=sum_send,
            recv_sem=sum_recv,
            device_id=(x, y),
            device_id_type=MESH,
        ).start()

    for_others(tell)
    others = sums.at[pl.ds(0, n_all - 1)]
    pltpu.make_async_copy(others, others, sum_recv).wait()
    totals = jnp.sum(sums[...], axis=0)
    value = {key: totals[:, k : k + 1] for k, key in enumerate(keys)}

    rho, g0, g1, g2 = value[(0, 0)], value[(0, 1)], value[(0, 2)], value[(0, 3)]
    a00, a01, a02 = value[(1, 1)], value[(1, 2)], value[(1, 3)]
    a11, a12, a22 = value[(2, 2)], value[(2, 3)], value[(3, 3)]
    l10, l20, y0 = a01 / a00, a02 / a00, g0 / a00
    d1, e12, f1 = a11 - l10 * a01, a12 - l10 * a02, g1 - l10 * g0
    l21, y1 = e12 / d1, f1 / d1
    d2, f2 = a22 - l20 * a02 - l21 * e12, g2 - l20 * g0 - l21 * f1
    y2 = f2 / d2
    norm0 = rho - y0 * g0
    norm1 = norm0 - y1 * f1
    norm2 = norm1 - y2 * f2
    y1 = y1 - l21 * y2
    y0 = y0 - l10 * y1 - l20 * y2
    y0, y1, y2 = [c.reshape(1, 1, 1) for c in (y0, y1, y2)]
    out_x[...] = y0 * fields[0] + y1 * fields[1] + y2 * fields[2]
    out_r[...] = r0[...] - y0 * images[0] - y1 * images[1] - y2 * images[2]
    norm_lane = lax.broadcasted_iota(jnp.int32, (1, levels), 1)
    norms = jnp.where(norm_lane == 0, norm0, jnp.where(norm_lane == 1, norm1, norm2))
    out_norms[...] = norms / total_cells

    for t in range(ITERS):
        wait_cols(east_border, col_send.at[t, 0])
        wait_cols(west_border, col_send.at[t, 1])

        @pl.when(has_north)
        def _(t=t):
            row_copy(t, 0).wait_send()

        @pl.when(has_south)
        def _(t=t):
            row_copy(t, 1).wait_send()

    pltpu.make_async_copy(others, others, sum_send).wait()


def on_device(n_gx, n_gy, right_side, diagonal, horizontal, vertical, precond, edge_rows):
    rows, cols, levels = right_side.shape
    f32 = jnp.float32
    block = (rows, cols, levels)
    sems = pltpu.SemaphoreType.DMA
    x, r, norms = pl.pallas_call(
        functools.partial(kernel, n_gx, n_gy),
        out_shape=(
            jax.ShapeDtypeStruct(block, f32),
            jax.ShapeDtypeStruct(block, f32),
            jax.ShapeDtypeStruct((1, levels), f32),
        ),
        in_specs=[SMEM, ANY, ANY, ANY, ANY, ANY],
        out_specs=(VMEM, VMEM, VMEM),
        scratch_shapes=[
            pltpu.VMEM(block, f32),
            pltpu.VMEM(block, f32),
            pltpu.VMEM(block, f32),
            pltpu.VMEM((1, levels), f32),
            pltpu.VMEM((levels, levels), f32),
            pltpu.VMEM((ITERS,) + block, f32),
            pltpu.VMEM((ITERS,) + block, f32),
            pltpu.VMEM((ITERS, 2, rows, 1, levels), f32),
            [pltpu.VMEM((n_gy * rows, 1, levels), f32)] * ITERS,
            [pltpu.VMEM((n_gy * rows, 1, levels), f32)] * ITERS,
            pltpu.VMEM((ITERS, cols, levels), f32),
            pltpu.VMEM((ITERS, cols, levels), f32),
            pltpu.VMEM((rows, 1, levels), f32),
            pltpu.VMEM((rows, 1, levels), f32),
            pltpu.VMEM((n_gx * n_gy, 1, levels), f32),
            sems((5,)),
            sems((ITERS, 2)),
            sems((ITERS,)),
            sems((ITERS,)),
            sems((ITERS, 2)),
            sems((ITERS,)),
            sems((ITERS,)),
            sems(()),
            sems(()),
        ],
        compiler_params=pltpu.CompilerParams(collective_id=0, has_side_effects=True),
    )(edge_rows, right_side, diagonal, horizontal, vertical.reshape(1, levels), precond)
    return x, r, norms[0, :ITERS]


def solution(mesh):
    n_gx, n_gy = mesh.shape["gx"], mesh.shape["gy"]
    field = P("gy", "gx", None)
    return jax.shard_map(
        functools.partial(on_device, n_gx, n_gy),
        mesh=mesh,
        in_specs=(field, field, field, P(), P(), P()),
        out_specs=(field, field, P()),
        check_vma=False,
    )
```

```python
import functools

import jax
import jax.numpy as jnp
from jax import lax
from jax.experimental import pallas as pl
from jax.experimental.pallas import tpu as pltpu
from jax.sharding import PartitionSpec as P

ITERS = 3
KEYS = [(i, j) for j in range(ITERS + 1) for i in range(j + 1)]
MESH = pl.DeviceIdType.MESH
ANY = pl.BlockSpec(memory_space=pl.ANY)
VMEM = pl.BlockSpec(memory_space=pltpu.VMEM)
SMEM = pl.BlockSpec(memory_space=pltpu.SMEM)


def kernel(
    n_gx,
    n_gy,
    edge_rows,
    right_side,
    diagonal,
    horizontal,
    vertical,
    precond,
    fields,
    images,
    out_totals,
    r0,
    diag,
    horiz,
    vert,
    matrix,
    send_cols,
    from_east,
    from_west,
    from_north,
    from_south,
    east_col,
    west_col,
    sums,
    load_sem,
    col_send,
    east_recv,
    west_recv,
    row_send,
    north_recv,
    south_recv,
    sum_send,
    sum_recv,
):
    rows, cols, levels = r0.shape
    gx, gy = lax.axis_index("gx"), lax.axis_index("gy")
    n_all = n_gx * n_gy
    half = n_gx // 2
    me = gx * n_gy + gy

    def for_others(visit):
        for j in range(1, n_gy):
            visit(gx, lax.rem(gy + j, n_gy))

        def step(i, carry):
            for j in range(n_gy):
                visit(lax.rem(gx + i, n_gx), lax.rem(gy + j, n_gy))
            return carry

        if n_all <= 64:
            for i in range(1, n_gx):
                step(i, 0)
        else:
            lax.fori_loop(1, n_gx, step, 0)

    barrier = pltpu.get_barrier_semaphore()

    def greet(x, y):
        pl.semaphore_signal(barrier, inc=1, device_id=(x, y), device_id_type=MESH)

    for_others(greet)

    panel = lax.convert_element_type(gx >= half, jnp.int32)
    loads = [
        pltpu.make_async_copy(right_side, r0, load_sem.at[0]),
        pltpu.make_async_copy(precond.at[panel], matrix, load_sem.at[1]),
        pltpu.make_async_copy(diagonal, diag, load_sem.at[2]),
        pltpu.make_async_copy(horizontal, horiz, load_sem.at[3]),
        pltpu.make_async_copy(vertical, vert, load_sem.at[4]),
    ]
    for load in loads:
        load.start()

    east_x, west_x = lax.rem(gx + 1, n_gx), lax.rem(gx + n_gx - 1, n_gx)
    east_border = (gx == half - 1) | (gx == n_gx - 1)
    west_border = (gx == half) | (gx == 0)
    east_table = jnp.where(gx == half - 1, 0, 1)
    west_table = jnp.where(gx == half, 0, 1)
    first_row = gy * rows
    has_north, has_south = gy < n_gy - 1, gy > 0

    @pl.when(jnp.logical_not(has_north))
    def _():
        from_north[...] = jnp.zeros_like(from_north)

    @pl.when(jnp.logical_not(has_south))
    def _():
        from_south[...] = jnp.zeros_like(from_south)

    def flat(v):
        return v.reshape(rows * cols, levels)

    def precondition(v):
        return lax.dot_general(
            flat(v),
            matrix[...],
            (((1,), (1,)), ((), ())),
            precision=lax.Precision.HIGHEST,
            preferred_element_type=jnp.float32,
        ).reshape(rows, cols, levels)

    def col_copy(t, side, g):
        buffer, recv, x = (
            (from_west, west_recv, east_x) if side == 0 else (from_east, east_recv, west_x)
        )
        return pltpu.make_async_remote_copy(
            src_ref=send_cols.at[t, side],
            dst_ref=buffer[t].at[pl.ds(first_row, rows)],
            send_sem=col_send.at[t, side],
            recv_sem=recv.at[t],
            device_id=(x, g),
            device_id_type=MESH,
        )

    def row_copy(t, side):
        buffer, recv, y, row = (
            (from_south, south_recv, gy + 1, rows - 1)
            if side == 0
            else (from_north, north_recv, gy - 1, 0)
        )
        return pltpu.make_async_remote_copy(
            src_ref=fields.at[t, row],
            dst_ref=buffer.at[t],
            send_sem=row_send.at[t, side],
            recv_sem=recv.at[t],
            device_id=(gx, y),
            device_id_type=MESH,
        )

    def send(t):
        for side, border in ((0, east_border), (1, west_border)):
            for g in range(n_gy):
                @pl.when(border | (gy == g))
                def _(side=side, g=g):
                    col_copy(t, side, g).start()

        @pl.when(has_north)
        def _():
            row_copy(t, 0).start()

        @pl.when(has_south)
        def _():
            row_copy(t, 1).start()

    def wait_cols(border, sem):
        whole = from_east[0]
        part = whole.at[pl.ds(0, rows)]

        @pl.when(border)
        def _():
            pltpu.make_async_copy(whole, whole, sem).wait()

        @pl.when(jnp.logical_not(border))
        def _():
            pltpu.make_async_copy(part, part, sem).wait()

    def receive(t):
        @pl.when(has_north)
        def _():
            row_copy(t, 1).wait_recv()

        @pl.when(has_south)
        def _():
            row_copy(t, 0).wait_recv()

        for border, recv, buffer, table, col in (
            (east_border, east_recv, from_east, east_table, east_col),
            (west_border, west_recv, from_west, west_table, west_col),
        ):
            wait_cols(border, recv.at[t])

            @pl.when(border)
            def _(buffer=buffer, table=table, col=col):
                for y in range(rows):
                    col[y] = buffer[t][edge_rows[table, first_row + y]]

            @pl.when(jnp.logical_not(border))
            def _(buffer=buffer, col=col):
                col[...] = buffer[t][pl.ds(first_row, rows)]

    col_id = lax.broadcasted_iota(jnp.int32, (rows, cols, levels), 1)
    lane_id = lax.broadcasted_iota(jnp.int32, (rows * cols, levels), 1)

    def local_part(z):
        flat_z = flat(z)
        up = jnp.where(lane_id < levels - 1, pltpu.roll(flat_z, levels - 1, 1), 0.0)
        down = jnp.where(lane_id > 0, pltpu.roll(flat_z, 1, 1), 0.0)
        column = (up + down).reshape(rows, cols, levels)
        v = vert[...].reshape(1, 1, levels)
        return diag[...] * z + v * (2.0 * z - column)

    def image_of(t, z, base):
        east = jnp.where(col_id == cols - 1, east_col[...], pltpu.roll(z, cols - 1, 1))
        west = jnp.where(col_id == 0, west_col[...], pltpu.roll(z, 1, 1))
        north = jnp.concatenate([z[1:], from_north[t][None]], 0)
        south = jnp.concatenate([from_south[t][None], z[:-1]], 0)
        return base + horiz[...] * (4.0 * z - (east + west + north + south))

    def product(a, b):
        both = (a * b).reshape(rows * cols // 8, 8, levels)
        return jnp.sum(jnp.sum(both, axis=0), axis=0, keepdims=True)

    loads[0].wait()
    loads[1].wait()
    terms = {}
    spaces = [r0]
    for t in range(ITERS):
        z = precondition(spaces[-1][...])
        fields[t] = z
        send_cols[t, 0] = z[:, cols - 1 : cols, :]
        send_cols[t, 1] = z[:, 0:1, :]
        if t == 0:
            pl.semaphore_wait(barrier, n_all - 1)
        send(t)
        if t == 0:
            for load in loads[2:]:
                load.wait()
        newest = len(spaces) - 1
        for i in range(len(spaces)):
            terms[(i, newest)] = product(spaces[i][...], spaces[newest][...])
        base = local_part(z)
        receive(t)
        images[t] = image_of(t, z, base)
        spaces.append(images.at[t])
    newest = len(spaces) - 1
    for i in range(len(spaces)):
        terms[(i, newest)] = product(spaces[i][...], spaces[newest][...])

    keys = KEYS
    height = -(-len(keys) // 8) * 8
    row_id = lax.broadcasted_iota(jnp.int32, (height, levels), 0)
    lane = lax.broadcasted_iota(jnp.int32, (height, levels), 1)
    stacked = jnp.zeros((height, levels), jnp.float32)
    for k, key in enumerate(keys):
        stacked = jnp.where(row_id == k, terms[key], stacked)
    summed = jnp.sum(stacked, axis=1, keepdims=True)
    sums[me] = jnp.sum(jnp.where(lane == row_id, summed, 0.0), axis=0, keepdims=True)

    def tell(x, y):
        pltpu.make_async_remote_copy(
            src_ref=sums.at[me],
            dst_ref=sums.at[me],
            send_sem=sum_send,
            recv_sem=sum_recv,
            device_id=(x, y),
            device_id_type=MESH,
        ).start()

    for_others(tell)
    others = sums.at[pl.ds(0, n_all - 1)]
    pltpu.make_async_copy(others, others, sum_recv).wait()
    out_totals[...] = jnp.sum(sums[...], axis=0)

    for t in range(ITERS):
        wait_cols(east_border, col_send.at[t, 0])
        wait_cols(west_border, col_send.at[t, 1])

        @pl.when(has_north)
        def _(t=t):
            row_copy(t, 0).wait_send()

        @pl.when(has_south)
        def _(t=t):
            row_copy(t, 1).wait_send()

    pltpu.make_async_copy(others, others, sum_send).wait()


def finish(total_cells, all_totals, r0, fields, images, out_x, out_r, out_norms, x, r, sem):
    levels = r0.shape[-1]
    totals = all_totals[...]
    value = {key: totals[:, k : k + 1] for k, key in enumerate(KEYS)}

    rho, g0, g1, g2 = value[(0, 0)], value[(0, 1)], value[(0, 2)], value[(0, 3)]
    a00, a01, a02 = value[(1, 1)], value[(1, 2)], value[(1, 3)]
    a11, a12, a22 = value[(2, 2)], value[(2, 3)], value[(3, 3)]
    l10, l20, y0 = a01 / a00, a02 / a00, g0 / a00
    d1, e12, f1 = a11 - l10 * a01, a12 - l10 * a02, g1 - l10 * g0
    l21, y1 = e12 / d1, f1 / d1
    d2, f2 = a22 - l20 * a02 - l21 * e12, g2 - l20 * g0 - l21 * f1
    y2 = f2 / d2
    norm0 = rho - y0 * g0
    norm1 = norm0 - y1 * f1
    norm2 = norm1 - y2 * f2
    y1 = y1 - l21 * y2
    y0 = y0 - l10 * y1 - l20 * y2
    y0, y1, y2 = [c.reshape(1, 1, 1) for c in (y0, y1, y2)]
    norm_lane = lax.broadcasted_iota(jnp.int32, (1, levels), 1)
    norms = jnp.where(norm_lane == 0, norm0, jnp.where(norm_lane == 1, norm1, norm2))
    out_norms[...] = norms[:, :ITERS] / total_cells
    rows = r0.shape[0]
    pieces = 2 if rows % 2 == 0 else 1
    size = rows // pieces
    copies = []
    for p in range(pieces):
        span = pl.ds(p * size, size)
        x[span] = y0 * fields[0, span] + y1 * fields[1, span] + y2 * fields[2, span]
        r[span] = (
            r0[span] - y0 * images[0, span] - y1 * images[1, span] - y2 * images[2, span]
        )
        for k, (src, dst) in enumerate(((x, out_x), (r, out_r))):
            copy = pltpu.make_async_copy(src.at[span], dst.at[span], sem.at[p, k])
            copy.start()
            copies.append(copy)
    for copy in copies:
        copy.wait()


def on_device(n_gx, n_gy, right_side, diagonal, horizontal, vertical, precond, edge_rows):
    rows, cols, levels = right_side.shape
    f32 = jnp.float32
    block = (rows, cols, levels)
    sems = pltpu.SemaphoreType.DMA
    basis = pltpu.VMEM((ITERS,) + block, f32)
    fields, images, totals, start = pl.pallas_call(
        functools.partial(kernel, n_gx, n_gy),
        out_shape=(basis, basis, pltpu.VMEM((1, levels), f32), pltpu.VMEM(block, f32)),
        in_specs=[SMEM, ANY, ANY, ANY, ANY, ANY],
        out_specs=(VMEM, VMEM, VMEM, VMEM),
        scratch_shapes=[
            pltpu.VMEM(block, f32),
            pltpu.VMEM(block, f32),
            pltpu.VMEM((1, levels), f32),
            pltpu.VMEM((levels, levels), f32),
            pltpu.VMEM((ITERS, 2, rows, 1, levels), f32),
            [pltpu.VMEM((n_gy * rows, 1, levels), f32)] * ITERS,
            [pltpu.VMEM((n_gy * rows, 1, levels), f32)] * ITERS,
            pltpu.VMEM((ITERS, cols, levels), f32),
            pltpu.VMEM((ITERS, cols, levels), f32),
            pltpu.VMEM((rows, 1, levels), f32),
            pltpu.VMEM((rows, 1, levels), f32),
            pltpu.VMEM((n_gx * n_gy, 1, levels), f32),
            sems((5,)),
            sems((ITERS, 2)),
            sems((ITERS,)),
            sems((ITERS,)),
            sems((ITERS, 2)),
            sems((ITERS,)),
            sems((ITERS,)),
            sems(()),
            sems(()),
        ],
        compiler_params=pltpu.CompilerParams(collective_id=0, has_side_effects=True),
    )(edge_rows, right_side, diagonal, horizontal, vertical.reshape(1, levels), precond)
    in_vmem = functools.partial(
        pltpu.with_memory_space_constraint, memory_space=pltpu.VMEM
    )
    total_cells = float(rows * cols * levels * n_gx * n_gy)
    x, r, norms = pl.pallas_call(
        functools.partial(finish, total_cells),
        out_shape=(
            jax.ShapeDtypeStruct(block, f32),
            jax.ShapeDtypeStruct(block, f32),
            jax.ShapeDtypeStruct((1, ITERS), f32),
        ),
        in_specs=[VMEM, VMEM, VMEM, VMEM],
        out_specs=(ANY, ANY, VMEM),
        scratch_shapes=[pltpu.VMEM(block, f32), pltpu.VMEM(block, f32), sems((2, 2))],
    )(in_vmem(totals), in_vmem(start), in_vmem(fields), in_vmem(images))
    return x, r, norms.reshape(ITERS)


def solution(mesh):
    n_gx, n_gy = mesh.shape["gx"], mesh.shape["gy"]
    field = P("gy", "gx", None)
    return jax.shard_map(
        functools.partial(on_device, n_gx, n_gy),
        mesh=mesh,
        in_specs=(field, field, field, P(), P(), P()),
        out_specs=(field, field, P()),
        check_vma=False,
    )
```

```python
import functools

import jax
import jax.numpy as jnp
from jax import lax
from jax.experimental import pallas as pl
from jax.experimental.pallas import tpu as pltpu
from jax.sharding import PartitionSpec as P

ITERS = 3
KEYS = [(i, j) for j in range(ITERS + 1) for i in range(j + 1)]
MESH = pl.DeviceIdType.MESH
ANY = pl.BlockSpec(memory_space=pl.ANY)
VMEM = pl.BlockSpec(memory_space=pltpu.VMEM)
SMEM = pl.BlockSpec(memory_space=pltpu.SMEM)


def kernel(
    n_gx,
    n_gy,
    out_rows,
    edge_rows,
    right_side,
    diagonal,
    horizontal,
    vertical,
    precond,
    fields,
    images,
    out_totals,
    r0,
    diag,
    horiz,
    vert,
    matrix,
    send_cols,
    from_east,
    from_west,
    from_north,
    from_south,
    outside,
    sums,
    load_sem,
    col_send,
    east_recv,
    west_recv,
    row_send,
    north_recv,
    south_recv,
    sum_send,
    sum_recv,
):
    rows, levels = out_rows, r0.shape[-1]
    cells = r0.shape[0]
    cols = cells // rows
    gx, gy = lax.axis_index("gx"), lax.axis_index("gy")
    n_all = n_gx * n_gy
    half = n_gx // 2
    me = gx * n_gy + gy

    def for_others(visit):
        for j in range(1, n_gy):
            visit(gx, lax.rem(gy + j, n_gy))

        def step(i, carry):
            for j in range(n_gy):
                visit(lax.rem(gx + i, n_gx), lax.rem(gy + j, n_gy))
            return carry

        if n_all <= 64:
            for i in range(1, n_gx):
                step(i, 0)
        else:
            lax.fori_loop(1, n_gx, step, 0)

    barrier = pltpu.get_barrier_semaphore()

    def greet(x, y):
        pl.semaphore_signal(barrier, inc=1, device_id=(x, y), device_id_type=MESH)

    for_others(greet)

    panel = lax.convert_element_type(gx >= half, jnp.int32)
    loads = [
        pltpu.make_async_copy(right_side, r0, load_sem.at[0]),
        pltpu.make_async_copy(precond.at[panel], matrix, load_sem.at[1]),
        pltpu.make_async_copy(diagonal, diag, load_sem.at[2]),
        pltpu.make_async_copy(horizontal, horiz, load_sem.at[3]),
        pltpu.make_async_copy(vertical, vert, load_sem.at[4]),
    ]
    for load in loads:
        load.start()

    east_x, west_x = lax.rem(gx + 1, n_gx), lax.rem(gx + n_gx - 1, n_gx)
    east_border = (gx == half - 1) | (gx == n_gx - 1)
    west_border = (gx == half) | (gx == 0)
    east_table = jnp.where(gx == half - 1, 0, 1)
    west_table = jnp.where(gx == half, 0, 1)
    first_row = gy * rows
    has_north, has_south = gy < n_gy - 1, gy > 0

    @pl.when(jnp.logical_not(has_north))
    def _():
        from_north[...] = jnp.zeros_like(from_north)

    @pl.when(jnp.logical_not(has_south))
    def _():
        from_south[...] = jnp.zeros_like(from_south)

    def precondition(v):
        return lax.dot_general(
            v,
            matrix[...],
            (((1,), (1,)), ((), ())),
            precision=lax.Precision.HIGHEST,
            preferred_element_type=jnp.float32,
        )

    def col_copy(t, side, g):
        buffer, recv, x = (
            (from_west, west_recv, east_x) if side == 0 else (from_east, east_recv, west_x)
        )
        return pltpu.make_async_remote_copy(
            src_ref=send_cols.at[t, pl.ds(side * rows, rows)],
            dst_ref=buffer[t].at[pl.ds(first_row, rows)],
            send_sem=col_send.at[t, side],
            recv_sem=recv.at[t],
            device_id=(x, g),
            device_id_type=MESH,
        )

    def row_copy(t, side):
        buffer, recv, y, row = (
            (from_south, south_recv, gy + 1, cells - cols)
            if side == 0
            else (from_north, north_recv, gy - 1, 0)
        )
        return pltpu.make_async_remote_copy(
            src_ref=fields.at[t, pl.ds(row, cols)],
            dst_ref=buffer.at[t],
            send_sem=row_send.at[t, side],
            recv_sem=recv.at[t],
            device_id=(gx, y),
            device_id_type=MESH,
        )

    def send_cols_on(t, edges):
        send_cols[t] = precondition(edges)
        if t == 0:
            pl.semaphore_wait(barrier, n_all - 1)
        for side, border in ((0, east_border), (1, west_border)):
            for g in range(n_gy):
                @pl.when(border | (gy == g))
                def _(side=side, g=g):
                    col_copy(t, side, g).start()

    def send_rows(t):
        @pl.when(has_north)
        def _():
            row_copy(t, 0).start()

        @pl.when(has_south)
        def _():
            row_copy(t, 1).start()

    def wait_cols(border, sem):
        whole = from_east[0]
        part = whole.at[pl.ds(0, rows)]

        @pl.when(border)
        def _():
            pltpu.make_async_copy(whole, whole, sem).wait()

        @pl.when(jnp.logical_not(border))
        def _():
            pltpu.make_async_copy(part, part, sem).wait()

    def receive_rows(t):
        @pl.when(has_north)
        def _():
            row_copy(t, 1).wait_recv()

        @pl.when(has_south)
        def _():
            row_copy(t, 0).wait_recv()

    def receive_cols(t):
        for border, recv, buffer, table, part in (
            (east_border, east_recv, from_east, east_table, 0),
            (west_border, west_recv, from_west, west_table, rows),
        ):
            wait_cols(border, recv.at[t])

            @pl.when(border)
            def _(buffer=buffer, table=table, part=part):
                for y in range(rows):
                    row = edge_rows[table, first_row + y]
                    outside[pl.ds(part + y, 1), :] = buffer[t][pl.ds(row, 1), :]

            @pl.when(jnp.logical_not(border))
            def _(buffer=buffer, part=part):
                outside[pl.ds(part, rows), :] = buffer[t][pl.ds(first_row, rows), :]

    col_id = lax.rem(lax.broadcasted_iota(jnp.int32, (cells, levels), 0), cols)
    lane_id = lax.broadcasted_iota(jnp.int32, (cells, levels), 1)
    east_edge = pl.ds(cols - 1, rows, stride=cols)
    west_edge = pl.ds(0, rows, stride=cols)
    south_edge = pl.ds(0, cols)
    north_edge = pl.ds(cells - cols, cols)

    def edge_columns(ref):
        return jnp.concatenate([ref[east_edge, :], ref[west_edge, :]], 0)

    def inner_image(z):
        up = jnp.where(lane_id < levels - 1, pltpu.roll(z, levels - 1, 1), 0.0)
        down = jnp.where(lane_id > 0, pltpu.roll(z, 1, 1), 0.0)
        east = jnp.where(col_id < cols - 1, pltpu.roll(z, cells - 1, 0), 0.0)
        west = jnp.where(col_id > 0, pltpu.roll(z, 1, 0), 0.0)
        none = jnp.zeros((cols, levels), jnp.float32)
        north = jnp.concatenate([z[cols:], none], 0)
        south = jnp.concatenate([none, z[:-cols]], 0)
        beside = east + west + north + south
        return (
            diag[...] * z
            + horiz[...] * (4.0 * z - beside)
            + vert[...] * (2.0 * z - (up + down))
        )

    def product(a, b):
        both = (a * b).reshape(cells // 8, 8, levels)
        return jnp.sum(jnp.sum(both, axis=0), axis=0, keepdims=True)

    loads[0].wait()
    loads[1].wait()
    terms = {}
    spaces = [r0]
    send_cols_on(0, edge_columns(r0))
    for t in range(ITERS):
        image = images.at[t]
        z = precondition(spaces[-1][...])
        fields[t] = z
        send_rows(t)
        if t == 0:
            for load in loads[2:]:
                load.wait()
            edge_horiz = edge_columns(horiz)
        newest = len(spaces) - 1
        for i in range(len(spaces)):
            terms[(i, newest)] = product(spaces[i][...], spaces[newest][...])
        image[...] = inner_image(z)
        receive_rows(t)
        image[south_edge, :] = image[south_edge, :] - horiz[south_edge, :] * from_south[t]
        image[north_edge, :] = image[north_edge, :] - horiz[north_edge, :] * from_north[t]
        inside = edge_columns(image)
        receive_cols(t)
        edges = inside - edge_horiz * outside[...]
        if t < ITERS - 1:
            send_cols_on(t + 1, edges)
        image[east_edge, :] = edges[:rows]
        image[west_edge, :] = edges[rows:]
        spaces.append(image)
    newest = len(spaces) - 1
    for i in range(len(spaces)):
        terms[(i, newest)] = product(spaces[i][...], spaces[newest][...])

    keys = KEYS
    height = -(-len(keys) // 8) * 8
    row_id = lax.broadcasted_iota(jnp.int32, (height, levels), 0)
    lane = lax.broadcasted_iota(jnp.int32, (height, levels), 1)
    stacked = jnp.zeros((height, levels), jnp.float32)
    for k, key in enumerate(keys):
        stacked = jnp.where(row_id == k, terms[key], stacked)
    summed = jnp.sum(stacked, axis=1, keepdims=True)
    sums[me] = jnp.sum(jnp.where(lane == row_id, summed, 0.0), axis=0, keepdims=True)

    def tell(x, y):
        pltpu.make_async_remote_copy(
            src_ref=sums.at[me],
            dst_ref=sums.at[me],
            send_sem=sum_send,
            recv_sem=sum_recv,
            device_id=(x, y),
            device_id_type=MESH,
        ).start()

    for_others(tell)
    others = sums.at[pl.ds(0, n_all - 1)]
    pltpu.make_async_copy(others, others, sum_recv).wait()
    out_totals[...] = jnp.sum(sums[...], axis=0)

    for t in range(ITERS):
        wait_cols(east_border, col_send.at[t, 0])
        wait_cols(west_border, col_send.at[t, 1])

        @pl.when(has_north)
        def _(t=t):
            row_copy(t, 0).wait_send()

        @pl.when(has_south)
        def _(t=t):
            row_copy(t, 1).wait_send()

    pltpu.make_async_copy(others, others, sum_send).wait()


def finish(total_cells, all_totals, r0, fields, images, out_x, out_r, out_norms, x, r, sem):
    levels = r0.shape[-1]
    totals = all_totals[...]
    value = {key: totals[:, k : k + 1] for k, key in enumerate(KEYS)}

    rho, g0, g1, g2 = value[(0, 0)], value[(0, 1)], value[(0, 2)], value[(0, 3)]
    a00, a01, a02 = value[(1, 1)], value[(1, 2)], value[(1, 3)]
    a11, a12, a22 = value[(2, 2)], value[(2, 3)], value[(3, 3)]
    l10, l20, y0 = a01 / a00, a02 / a00, g0 / a00
    d1, e12, f1 = a11 - l10 * a01, a12 - l10 * a02, g1 - l10 * g0
    l21, y1 = e12 / d1, f1 / d1
    d2, f2 = a22 - l20 * a02 - l21 * e12, g2 - l20 * g0 - l21 * f1
    y2 = f2 / d2
    norm0 = rho - y0 * g0
    norm1 = norm0 - y1 * f1
    norm2 = norm1 - y2 * f2
    y1 = y1 - l21 * y2
    y0 = y0 - l10 * y1 - l20 * y2
    norm_lane = lax.broadcasted_iota(jnp.int32, (1, levels), 1)
    norms = jnp.where(norm_lane == 0, norm0, jnp.where(norm_lane == 1, norm1, norm2))
    out_norms[...] = norms[:, :ITERS] / total_cells
    rows = r0.shape[0]
    pieces = 2 if rows % 16 == 0 else 1
    size = rows // pieces
    copies = []
    for p in range(pieces):
        span = pl.ds(p * size, size)
        x[span] = y0 * fields[0, span] + y1 * fields[1, span] + y2 * fields[2, span]
        r[span] = (
            r0[span] - y0 * images[0, span] - y1 * images[1, span] - y2 * images[2, span]
        )
        for k, (src, dst) in enumerate(((x, out_x), (r, out_r))):
            copy = pltpu.make_async_copy(src.at[span], dst.at[span], sem.at[p, k])
            copy.start()
            copies.append(copy)
    for copy in copies:
        copy.wait()


def on_device(n_gx, n_gy, right_side, diagonal, horizontal, vertical, precond, edge_rows):
    rows, cols, levels = right_side.shape
    f32 = jnp.float32
    block = (rows * cols, levels)
    sems = pltpu.SemaphoreType.DMA
    basis = pltpu.VMEM((ITERS,) + block, f32)
    fields, images, totals, start = pl.pallas_call(
        functools.partial(kernel, n_gx, n_gy, rows),
        out_shape=(basis, basis, pltpu.VMEM((1, levels), f32), pltpu.VMEM(block, f32)),
        in_specs=[SMEM, ANY, ANY, ANY, ANY, ANY],
        out_specs=(VMEM, VMEM, VMEM, VMEM),
        scratch_shapes=[
            pltpu.VMEM(block, f32),
            pltpu.VMEM(block, f32),
            pltpu.VMEM((1, levels), f32),
            pltpu.VMEM((levels, levels), f32),
            pltpu.VMEM((ITERS, 2 * rows, levels), f32),
            [pltpu.VMEM((n_gy * rows, levels), f32)] * ITERS,
            [pltpu.VMEM((n_gy * rows, levels), f32)] * ITERS,
            pltpu.VMEM((ITERS, cols, levels), f32),
            pltpu.VMEM((ITERS, cols, levels), f32),
            pltpu.VMEM((2 * rows, levels), f32),
            pltpu.VMEM((n_gx * n_gy, 1, levels), f32),
            sems((5,)),
            sems((ITERS, 2)),
            sems((ITERS,)),
            sems((ITERS,)),
            sems((ITERS, 2)),
            sems((ITERS,)),
            sems((ITERS,)),
            sems(()),
            sems(()),
        ],
        compiler_params=pltpu.CompilerParams(collective_id=0, has_side_effects=True),
    )(
        edge_rows,
        right_side.reshape(block),
        diagonal.reshape(block),
        horizontal.reshape(block),
        vertical.reshape(1, levels),
        precond,
    )
    in_vmem = functools.partial(
        pltpu.with_memory_space_constraint, memory_space=pltpu.VMEM
    )
    total_cells = float(rows * cols * levels * n_gx * n_gy)
    x, r, norms = pl.pallas_call(
        functools.partial(finish, total_cells),
        out_shape=(
            jax.ShapeDtypeStruct(block, f32),
            jax.ShapeDtypeStruct(block, f32),
            jax.ShapeDtypeStruct((1, ITERS), f32),
        ),
        in_specs=[VMEM, VMEM, VMEM, VMEM],
        out_specs=(ANY, ANY, VMEM),
        scratch_shapes=[pltpu.VMEM(block, f32), pltpu.VMEM(block, f32), sems((2, 2))],
    )(in_vmem(totals), in_vmem(start), in_vmem(fields), in_vmem(images))
    shape = right_side.shape
    return x.reshape(shape), r.reshape(shape), norms.reshape(ITERS)


def solution(mesh):
    n_gx, n_gy = mesh.shape["gx"], mesh.shape["gy"]
    field = P("gy", "gx", None)
    return jax.shard_map(
        functools.partial(on_device, n_gx, n_gy),
        mesh=mesh,
        in_specs=(field, field, field, P(), P(), P()),
        out_specs=(field, field, P()),
        check_vma=False,
    )
```

```python
import functools

import jax
import jax.numpy as jnp
from jax import lax
from jax.experimental import pallas as pl
from jax.experimental.pallas import tpu as pltpu
from jax.sharding import PartitionSpec as P

ITERS = 3
KEYS = [(i, j) for j in range(ITERS + 1) for i in range(j + 1)]
MESH = pl.DeviceIdType.MESH
ANY = pl.BlockSpec(memory_space=pl.ANY)
VMEM = pl.BlockSpec(memory_space=pltpu.VMEM)


def kernel(
    n_gx,
    n_gy,
    out_rows,
    edge_table,
    right_side,
    diagonal,
    horizontal,
    vertical,
    precond,
    fields,
    images,
    out_totals,
    r0,
    diag,
    horiz,
    vert,
    matrix,
    send_cols,
    from_east,
    from_west,
    from_north,
    from_south,
    outside,
    sums,
    edge_rows,
    load_sem,
    col_send,
    east_recv,
    west_recv,
    row_send,
    north_recv,
    south_recv,
    sum_send,
    sum_recv,
):
    rows, levels = out_rows, r0.shape[-1]
    cells = r0.shape[0]
    cols = cells // rows
    gx, gy = lax.axis_index("gx"), lax.axis_index("gy")
    n_all = n_gx * n_gy
    half = n_gx // 2
    me = gx * n_gy + gy

    def for_others(visit):
        for j in range(1, n_gy):
            visit(gx, lax.rem(gy + j, n_gy))

        def step(i, carry):
            for j in range(n_gy):
                visit(lax.rem(gx + i, n_gx), lax.rem(gy + j, n_gy))
            return carry

        if n_all <= 64:
            for i in range(1, n_gx):
                step(i, 0)
        else:
            lax.fori_loop(1, n_gx, step, 0)

    barrier = pltpu.get_barrier_semaphore()

    def greet(x, y):
        pl.semaphore_signal(barrier, inc=1, device_id=(x, y), device_id_type=MESH)

    for_others(greet)

    panel = lax.convert_element_type(gx >= half, jnp.int32)
    loads = [
        pltpu.make_async_copy(right_side, r0, load_sem.at[0]),
        pltpu.make_async_copy(precond.at[panel], matrix, load_sem.at[1]),
        pltpu.make_async_copy(diagonal, diag, load_sem.at[2]),
        pltpu.make_async_copy(horizontal, horiz, load_sem.at[3]),
        pltpu.make_async_copy(vertical, vert, load_sem.at[4]),
        pltpu.make_async_copy(edge_table, edge_rows, load_sem.at[5]),
    ]
    for load in loads:
        load.start()

    east_x, west_x = lax.rem(gx + 1, n_gx), lax.rem(gx + n_gx - 1, n_gx)
    east_border = (gx == half - 1) | (gx == n_gx - 1)
    west_border = (gx == half) | (gx == 0)
    east_table = jnp.where(gx == half - 1, 0, 1)
    west_table = jnp.where(gx == half, 0, 1)
    first_row = gy * rows
    has_north, has_south = gy < n_gy - 1, gy > 0

    @pl.when(jnp.logical_not(has_north))
    def _():
        from_north[...] = jnp.zeros_like(from_north)

    @pl.when(jnp.logical_not(has_south))
    def _():
        from_south[...] = jnp.zeros_like(from_south)

    def precondition(v):
        return lax.dot_general(
            v,
            matrix[...],
            (((1,), (1,)), ((), ())),
            precision=lax.Precision.HIGHEST,
            preferred_element_type=jnp.float32,
        )

    def col_copy(t, side, g):
        buffer, recv, x = (
            (from_west, west_recv, east_x) if side == 0 else (from_east, east_recv, west_x)
        )
        return pltpu.make_async_remote_copy(
            src_ref=send_cols.at[t, pl.ds(side * rows, rows)],
            dst_ref=buffer[t].at[pl.ds(first_row, rows)],
            send_sem=col_send.at[t, side],
            recv_sem=recv.at[t],
            device_id=(x, g),
            device_id_type=MESH,
        )

    def row_copy(t, side):
        buffer, recv, y, row = (
            (from_south, south_recv, gy + 1, cells - cols)
            if side == 0
            else (from_north, north_recv, gy - 1, 0)
        )
        return pltpu.make_async_remote_copy(
            src_ref=fields.at[t, pl.ds(row, cols)],
            dst_ref=buffer.at[t],
            send_sem=row_send.at[t, side],
            recv_sem=recv.at[t],
            device_id=(gx, y),
            device_id_type=MESH,
        )

    def send_cols_on(t, edges):
        send_cols[t] = precondition(edges)
        if t == 0:
            pl.semaphore_wait(barrier, n_all - 1)
        for side, border in ((0, east_border), (1, west_border)):
            for g in range(n_gy):
                @pl.when(border | (gy == g))
                def _(side=side, g=g):
                    col_copy(t, side, g).start()

    def send_rows(t):
        @pl.when(has_north)
        def _():
            row_copy(t, 0).start()

        @pl.when(has_south)
        def _():
            row_copy(t, 1).start()

    def wait_cols(border, sem):
        whole = from_east[0]
        part = whole.at[pl.ds(0, rows)]

        @pl.when(border)
        def _():
            pltpu.make_async_copy(whole, whole, sem).wait()

        @pl.when(jnp.logical_not(border))
        def _():
            pltpu.make_async_copy(part, part, sem).wait()

    def receive_rows(t):
        @pl.when(has_north)
        def _():
            row_copy(t, 1).wait_recv()

        @pl.when(has_south)
        def _():
            row_copy(t, 0).wait_recv()

    def receive_cols(t):
        for border, recv, buffer, table, part in (
            (east_border, east_recv, from_east, east_table, 0),
            (west_border, west_recv, from_west, west_table, rows),
        ):
            wait_cols(border, recv.at[t])

            @pl.when(border)
            def _(buffer=buffer, table=table, part=part):
                for y in range(rows):
                    row = edge_rows[table, first_row + y]
                    outside[pl.ds(part + y, 1), :] = buffer[t][pl.ds(row, 1), :]

            @pl.when(jnp.logical_not(border))
            def _(buffer=buffer, part=part):
                outside[pl.ds(part, rows), :] = buffer[t][pl.ds(first_row, rows), :]

    col_id = lax.rem(lax.broadcasted_iota(jnp.int32, (cells, levels), 0), cols)
    lane_id = lax.broadcasted_iota(jnp.int32, (cells, levels), 1)
    east_edge = pl.ds(cols - 1, rows, stride=cols)
    west_edge = pl.ds(0, rows, stride=cols)
    south_edge = pl.ds(0, cols)
    north_edge = pl.ds(cells - cols, cols)

    def edge_columns(ref):
        return jnp.concatenate([ref[east_edge, :], ref[west_edge, :]], 0)

    def inner_image(z):
        up = jnp.where(lane_id < levels - 1, pltpu.roll(z, levels - 1, 1), 0.0)
        down = jnp.where(lane_id > 0, pltpu.roll(z, 1, 1), 0.0)
        east = jnp.where(col_id < cols - 1, pltpu.roll(z, cells - 1, 0), 0.0)
        west = jnp.where(col_id > 0, pltpu.roll(z, 1, 0), 0.0)
        none = jnp.zeros((cols, levels), jnp.float32)
        north = jnp.concatenate([z[cols:], none], 0)
        south = jnp.concatenate([none, z[:-cols]], 0)
        beside = east + west + north + south
        return (
            diag[...] * z
            + horiz[...] * (4.0 * z - beside)
            + vert[...] * (2.0 * z - (up + down))
        )

    def product(a, b):
        both = (a * b).reshape(cells // 8, 8, levels)
        return jnp.sum(jnp.sum(both, axis=0), axis=0, keepdims=True)

    loads[0].wait()
    loads[1].wait()
    terms = {}
    spaces = [r0]
    send_cols_on(0, edge_columns(r0))
    for t in range(ITERS):
        image = images.at[t]
        z = precondition(spaces[-1][...])
        fields[t] = z
        send_rows(t)
        if t == 0:
            for load in loads[2:]:
                load.wait()
            edge_horiz = edge_columns(horiz)
        newest = len(spaces) - 1
        for i in range(len(spaces)):
            terms[(i, newest)] = product(spaces[i][...], spaces[newest][...])
        image[...] = inner_image(z)
        receive_rows(t)
        image[south_edge, :] = image[south_edge, :] - horiz[south_edge, :] * from_south[t]
        image[north_edge, :] = image[north_edge, :] - horiz[north_edge, :] * from_north[t]
        inside = edge_columns(image)
        receive_cols(t)
        edges = inside - edge_horiz * outside[...]
        if t < ITERS - 1:
            send_cols_on(t + 1, edges)
        image[east_edge, :] = edges[:rows]
        image[west_edge, :] = edges[rows:]
        spaces.append(image)
    newest = len(spaces) - 1
    for i in range(len(spaces)):
        terms[(i, newest)] = product(spaces[i][...], spaces[newest][...])

    keys = KEYS
    height = -(-len(keys) // 8) * 8
    row_id = lax.broadcasted_iota(jnp.int32, (height, levels), 0)
    lane = lax.broadcasted_iota(jnp.int32, (height, levels), 1)
    stacked = jnp.zeros((height, levels), jnp.float32)
    for k, key in enumerate(keys):
        stacked = jnp.where(row_id == k, terms[key], stacked)
    summed = jnp.sum(stacked, axis=1, keepdims=True)
    sums[me] = jnp.sum(jnp.where(lane == row_id, summed, 0.0), axis=0, keepdims=True)

    def tell(x, y):
        pltpu.make_async_remote_copy(
            src_ref=sums.at[me],
            dst_ref=sums.at[me],
            send_sem=sum_send,
            recv_sem=sum_recv,
            device_id=(x, y),
            device_id_type=MESH,
        ).start()

    for_others(tell)
    others = sums.at[pl.ds(0, n_all - 1)]
    pltpu.make_async_copy(others, others, sum_recv).wait()
    out_totals[...] = jnp.sum(sums[...], axis=0)

    for t in range(ITERS):
        wait_cols(east_border, col_send.at[t, 0])
        wait_cols(west_border, col_send.at[t, 1])

        @pl.when(has_north)
        def _(t=t):
            row_copy(t, 0).wait_send()

        @pl.when(has_south)
        def _(t=t):
            row_copy(t, 1).wait_send()

    pltpu.make_async_copy(others, others, sum_send).wait()


def finish(total_cells, all_totals, r0, fields, images, out_x, out_r, out_norms, x, r, sem):
    levels = r0.shape[-1]
    totals = all_totals[...]
    value = {key: totals[:, k : k + 1] for k, key in enumerate(KEYS)}

    rho, g0, g1, g2 = value[(0, 0)], value[(0, 1)], value[(0, 2)], value[(0, 3)]
    a00, a01, a02 = value[(1, 1)], value[(1, 2)], value[(1, 3)]
    a11, a12, a22 = value[(2, 2)], value[(2, 3)], value[(3, 3)]
    l10, l20, y0 = a01 / a00, a02 / a00, g0 / a00
    d1, e12, f1 = a11 - l10 * a01, a12 - l10 * a02, g1 - l10 * g0
    l21, y1 = e12 / d1, f1 / d1
    d2, f2 = a22 - l20 * a02 - l21 * e12, g2 - l20 * g0 - l21 * f1
    y2 = f2 / d2
    norm0 = rho - y0 * g0
    norm1 = norm0 - y1 * f1
    norm2 = norm1 - y2 * f2
    y1 = y1 - l21 * y2
    y0 = y0 - l10 * y1 - l20 * y2
    norm_lane = lax.broadcasted_iota(jnp.int32, (1, levels), 1)
    norms = jnp.where(norm_lane == 0, norm0, jnp.where(norm_lane == 1, norm1, norm2))
    out_norms[...] = norms[:, :ITERS] / total_cells
    rows = r0.shape[0]
    pieces = 2 if rows % 16 == 0 else 1
    size = rows // pieces
    copies = []
    for p in range(pieces):
        span = pl.ds(p * size, size)
        x[span] = y0 * fields[0, span] + y1 * fields[1, span] + y2 * fields[2, span]
        r[span] = (
            r0[span] - y0 * images[0, span] - y1 * images[1, span] - y2 * images[2, span]
        )
        for k, (src, dst) in enumerate(((x, out_x), (r, out_r))):
            copy = pltpu.make_async_copy(src.at[span], dst.at[span], sem.at[p, k])
            copy.start()
            copies.append(copy)
    for copy in copies:
        copy.wait()


def on_device(n_gx, n_gy, right_side, diagonal, horizontal, vertical, precond, edge_rows):
    rows, cols, levels = right_side.shape
    f32 = jnp.float32
    block = (rows * cols, levels)
    sems = pltpu.SemaphoreType.DMA
    basis = pltpu.VMEM((ITERS,) + block, f32)
    fields, images, totals, start = pl.pallas_call(
        functools.partial(kernel, n_gx, n_gy, rows),
        out_shape=(basis, basis, pltpu.VMEM((1, levels), f32), pltpu.VMEM(block, f32)),
        in_specs=[ANY, ANY, ANY, ANY, ANY, ANY],
        out_specs=(VMEM, VMEM, VMEM, VMEM),
        scratch_shapes=[
            pltpu.VMEM(block, f32),
            pltpu.VMEM(block, f32),
            pltpu.VMEM((1, levels), f32),
            pltpu.VMEM((levels, levels), f32),
            pltpu.VMEM((ITERS, 2 * rows, levels), f32),
            [pltpu.VMEM((n_gy * rows, levels), f32)] * ITERS,
            [pltpu.VMEM((n_gy * rows, levels), f32)] * ITERS,
            pltpu.VMEM((ITERS, cols, levels), f32),
            pltpu.VMEM((ITERS, cols, levels), f32),
            pltpu.VMEM((2 * rows, levels), f32),
            pltpu.VMEM((n_gx * n_gy, 1, levels), f32),
            pltpu.SMEM(edge_rows.shape, jnp.int32),
            sems((6,)),
            sems((ITERS, 2)),
            sems((ITERS,)),
            sems((ITERS,)),
            sems((ITERS, 2)),
            sems((ITERS,)),
            sems((ITERS,)),
            sems(()),
            sems(()),
        ],
        compiler_params=pltpu.CompilerParams(collective_id=0, has_side_effects=True),
    )(
        edge_rows,
        right_side.reshape(block),
        diagonal.reshape(block),
        horizontal.reshape(block),
        vertical.reshape(1, levels),
        precond,
    )
    in_vmem = functools.partial(
        pltpu.with_memory_space_constraint, memory_space=pltpu.VMEM
    )
    total_cells = float(rows * cols * levels * n_gx * n_gy)
    x, r, norms = pl.pallas_call(
        functools.partial(finish, total_cells),
        out_shape=(
            jax.ShapeDtypeStruct(block, f32),
            jax.ShapeDtypeStruct(block, f32),
            jax.ShapeDtypeStruct((1, ITERS), f32),
        ),
        in_specs=[VMEM, VMEM, VMEM, VMEM],
        out_specs=(ANY, ANY, VMEM),
        scratch_shapes=[pltpu.VMEM(block, f32), pltpu.VMEM(block, f32), sems((2, 2))],
    )(in_vmem(totals), in_vmem(start), in_vmem(fields), in_vmem(images))
    shape = right_side.shape
    return x.reshape(shape), r.reshape(shape), norms.reshape(ITERS)


def solution(mesh):
    n_gx, n_gy = mesh.shape["gx"], mesh.shape["gy"]
    field = P("gy", "gx", None)
    return jax.shard_map(
        functools.partial(on_device, n_gx, n_gy),
        mesh=mesh,
        in_specs=(field, field, field, P(), P(), P()),
        out_specs=(field, field, P()),
        check_vma=False,
    )
```

```python
import functools

import jax
import jax.numpy as jnp
from jax import lax
from jax.experimental import pallas as pl
from jax.experimental.pallas import tpu as pltpu
from jax.sharding import PartitionSpec as P

ITERS = 3
KEYS = [(i, j) for j in range(ITERS + 1) for i in range(j + 1)]
MESH = pl.DeviceIdType.MESH
ANY = pl.BlockSpec(memory_space=pl.ANY)
VMEM = pl.BlockSpec(memory_space=pltpu.VMEM)


def kernel(
    n_gx,
    n_gy,
    out_rows,
    edge_table,
    right_side,
    diagonal,
    horizontal,
    vertical,
    precond,
    fields,
    images,
    out_totals,
    r0,
    diag,
    horiz,
    vert,
    matrix,
    send_cols,
    from_east,
    from_west,
    from_north,
    from_south,
    outside,
    sums,
    edge_rows,
    load_sem,
    col_send,
    east_recv,
    west_recv,
    row_send,
    north_recv,
    south_recv,
    sum_send,
    sum_recv,
):
    rows, levels = out_rows, r0.shape[-1]
    cells = r0.shape[0]
    cols = cells // rows
    gx, gy = lax.axis_index("gx"), lax.axis_index("gy")
    n_all = n_gx * n_gy
    half = n_gx // 2
    me = gx * n_gy + gy

    def for_others(visit):
        def step(i, carry):
            for j in range(n_gy):
                visit(lax.rem(gx + i, n_gx), lax.rem(gy + j, n_gy))
            return carry

        if n_all <= 64:
            for i in sorted(range(1, n_gx), key=lambda i: min(i, n_gx - i)):
                step(i, 0)
        else:
            lax.fori_loop(1, n_gx, step, 0)
        for j in range(1, n_gy):
            visit(gx, lax.rem(gy + j, n_gy))

    barrier = pltpu.get_barrier_semaphore()

    def greet(x, y):
        pl.semaphore_signal(barrier, inc=1, device_id=(x, y), device_id_type=MESH)

    for_others(greet)

    panel = lax.convert_element_type(gx >= half, jnp.int32)
    loads = [
        pltpu.make_async_copy(right_side, r0, load_sem.at[0]),
        pltpu.make_async_copy(precond.at[panel], matrix, load_sem.at[1]),
        pltpu.make_async_copy(diagonal, diag, load_sem.at[2]),
        pltpu.make_async_copy(horizontal, horiz, load_sem.at[3]),
        pltpu.make_async_copy(vertical, vert, load_sem.at[4]),
        pltpu.make_async_copy(edge_table, edge_rows, load_sem.at[5]),
    ]
    for load in loads:
        load.start()

    east_x, west_x = lax.rem(gx + 1, n_gx), lax.rem(gx + n_gx - 1, n_gx)
    east_border = (gx == half - 1) | (gx == n_gx - 1)
    west_border = (gx == half) | (gx == 0)
    east_table = jnp.where(gx == half - 1, 0, 1)
    west_table = jnp.where(gx == half, 0, 1)
    first_row = gy * rows
    has_north, has_south = gy < n_gy - 1, gy > 0

    @pl.when(jnp.logical_not(has_north))
    def _():
        from_north[...] = jnp.zeros_like(from_north)

    @pl.when(jnp.logical_not(has_south))
    def _():
        from_south[...] = jnp.zeros_like(from_south)

    def precondition(v):
        return lax.dot_general(
            v,
            matrix[...],
            (((1,), (1,)), ((), ())),
            precision=lax.Precision.HIGHEST,
            preferred_element_type=jnp.float32,
        )

    def col_copy(t, side, g):
        buffer, recv, x = (
            (from_west, west_recv, east_x) if side == 0 else (from_east, east_recv, west_x)
        )
        return pltpu.make_async_remote_copy(
            src_ref=send_cols.at[t, pl.ds(side * rows, rows)],
            dst_ref=buffer[t].at[pl.ds(first_row, rows)],
            send_sem=col_send.at[t, side],
            recv_sem=recv.at[t],
            device_id=(x, g),
            device_id_type=MESH,
        )

    def row_copy(t, side):
        buffer, recv, y, row = (
            (from_south, south_recv, gy + 1, cells - cols)
            if side == 0
            else (from_north, north_recv, gy - 1, 0)
        )
        return pltpu.make_async_remote_copy(
            src_ref=fields.at[t, pl.ds(row, cols)],
            dst_ref=buffer.at[t],
            send_sem=row_send.at[t, side],
            recv_sem=recv.at[t],
            device_id=(gx, y),
            device_id_type=MESH,
        )

    def send_cols_on(t, edges):
        send_cols[t] = precondition(edges)
        if t == 0:
            pl.semaphore_wait(barrier, n_all - 1)
        for side, border in ((0, east_border), (1, west_border)):
            @pl.when(border)
            def _(side=side):
                for j in sorted(range(1, n_gy), key=lambda j: abs(2 * j - n_gy)):
                    col_copy(t, side, lax.rem(gy + j, n_gy)).start()

            col_copy(t, side, gy).start()

    def send_rows(t):
        @pl.when(has_north)
        def _():
            row_copy(t, 0).start()

        @pl.when(has_south)
        def _():
            row_copy(t, 1).start()

    def wait_cols(border, sem):
        whole = from_east[0]
        part = whole.at[pl.ds(0, rows)]

        @pl.when(border)
        def _():
            pltpu.make_async_copy(whole, whole, sem).wait()

        @pl.when(jnp.logical_not(border))
        def _():
            pltpu.make_async_copy(part, part, sem).wait()

    def receive_rows(t):
        @pl.when(has_north)
        def _():
            row_copy(t, 1).wait_recv()

        @pl.when(has_south)
        def _():
            row_copy(t, 0).wait_recv()

    def receive_cols(t):
        for border, recv, buffer, table, part in (
            (east_border, east_recv, from_east, east_table, 0),
            (west_border, west_recv, from_west, west_table, rows),
        ):
            wait_cols(border, recv.at[t])

            @pl.when(border)
            def _(buffer=buffer, table=table, part=part):
                for y in range(rows):
                    row = edge_rows[table, first_row + y]
                    outside[pl.ds(part + y, 1), :] = buffer[t][pl.ds(row, 1), :]

            @pl.when(jnp.logical_not(border))
            def _(buffer=buffer, part=part):
                outside[pl.ds(part, rows), :] = buffer[t][pl.ds(first_row, rows), :]

    col_id = lax.rem(lax.broadcasted_iota(jnp.int32, (cells, levels), 0), cols)
    lane_id = lax.broadcasted_iota(jnp.int32, (cells, levels), 1)
    east_edge = pl.ds(cols - 1, rows, stride=cols)
    west_edge = pl.ds(0, rows, stride=cols)
    south_edge = pl.ds(0, cols)
    north_edge = pl.ds(cells - cols, cols)

    def edge_columns(ref):
        return jnp.concatenate([ref[east_edge, :], ref[west_edge, :]], 0)

    def inner_image(z):
        up = jnp.where(lane_id < levels - 1, pltpu.roll(z, levels - 1, 1), 0.0)
        down = jnp.where(lane_id > 0, pltpu.roll(z, 1, 1), 0.0)
        east = jnp.where(col_id < cols - 1, pltpu.roll(z, cells - 1, 0), 0.0)
        west = jnp.where(col_id > 0, pltpu.roll(z, 1, 0), 0.0)
        none = jnp.zeros((cols, levels), jnp.float32)
        north = jnp.concatenate([z[cols:], none], 0)
        south = jnp.concatenate([none, z[:-cols]], 0)
        beside = east + west + north + south
        return (
            diag[...] * z
            + horiz[...] * (4.0 * z - beside)
            + vert[...] * (2.0 * z - (up + down))
        )

    def product(a, b):
        both = (a * b).reshape(cells // 8, 8, levels)
        return jnp.sum(jnp.sum(both, axis=0), axis=0, keepdims=True)

    loads[0].wait()
    loads[1].wait()
    terms = {}
    spaces = [r0]
    send_cols_on(0, edge_columns(r0))
    for t in range(ITERS):
        image = images.at[t]
        z = precondition(spaces[-1][...])
        fields[t] = z
        send_rows(t)
        if t == 0:
            for load in loads[2:]:
                load.wait()
            edge_horiz = edge_columns(horiz)
        newest = len(spaces) - 1
        for i in range(len(spaces)):
            terms[(i, newest)] = product(spaces[i][...], spaces[newest][...])
        image[...] = inner_image(z)
        receive_rows(t)
        image[south_edge, :] = image[south_edge, :] - horiz[south_edge, :] * from_south[t]
        image[north_edge, :] = image[north_edge, :] - horiz[north_edge, :] * from_north[t]
        inside = edge_columns(image)
        receive_cols(t)
        edges = inside - edge_horiz * outside[...]
        if t < ITERS - 1:
            send_cols_on(t + 1, edges)
        image[east_edge, :] = edges[:rows]
        image[west_edge, :] = edges[rows:]
        spaces.append(image)
    newest = len(spaces) - 1
    for i in range(len(spaces)):
        terms[(i, newest)] = product(spaces[i][...], spaces[newest][...])

    keys = KEYS
    height = -(-len(keys) // 8) * 8
    row_id = lax.broadcasted_iota(jnp.int32, (height, levels), 0)
    lane = lax.broadcasted_iota(jnp.int32, (height, levels), 1)
    stacked = jnp.zeros((height, levels), jnp.float32)
    for k, key in enumerate(keys):
        stacked = jnp.where(row_id == k, terms[key], stacked)
    summed = jnp.sum(stacked, axis=1, keepdims=True)
    sums[me] = jnp.sum(jnp.where(lane == row_id, summed, 0.0), axis=0, keepdims=True)

    def tell(x, y):
        pltpu.make_async_remote_copy(
            src_ref=sums.at[me],
            dst_ref=sums.at[me],
            send_sem=sum_send,
            recv_sem=sum_recv,
            device_id=(x, y),
            device_id_type=MESH,
        ).start()

    for_others(tell)
    others = sums.at[pl.ds(0, n_all - 1)]
    pltpu.make_async_copy(others, others, sum_recv).wait()
    out_totals[...] = jnp.sum(sums[...], axis=0)

    for t in range(ITERS):
        wait_cols(east_border, col_send.at[t, 0])
        wait_cols(west_border, col_send.at[t, 1])

        @pl.when(has_north)
        def _(t=t):
            row_copy(t, 0).wait_send()

        @pl.when(has_south)
        def _(t=t):
            row_copy(t, 1).wait_send()

    pltpu.make_async_copy(others, others, sum_send).wait()


def finish(total_cells, all_totals, r0, fields, images, out_x, out_r, out_norms, x, r, sem):
    levels = r0.shape[-1]
    totals = all_totals[...]
    value = {key: totals[:, k : k + 1] for k, key in enumerate(KEYS)}

    rho, g0, g1, g2 = value[(0, 0)], value[(0, 1)], value[(0, 2)], value[(0, 3)]
    a00, a01, a02 = value[(1, 1)], value[(1, 2)], value[(1, 3)]
    a11, a12, a22 = value[(2, 2)], value[(2, 3)], value[(3, 3)]
    l10, l20, y0 = a01 / a00, a02 / a00, g0 / a00
    d1, e12, f1 = a11 - l10 * a01, a12 - l10 * a02, g1 - l10 * g0
    l21, y1 = e12 / d1, f1 / d1
    d2, f2 = a22 - l20 * a02 - l21 * e12, g2 - l20 * g0 - l21 * f1
    y2 = f2 / d2
    norm0 = rho - y0 * g0
    norm1 = norm0 - y1 * f1
    norm2 = norm1 - y2 * f2
    y1 = y1 - l21 * y2
    y0 = y0 - l10 * y1 - l20 * y2
    norm_lane = lax.broadcasted_iota(jnp.int32, (1, levels), 1)
    norms = jnp.where(norm_lane == 0, norm0, jnp.where(norm_lane == 1, norm1, norm2))
    out_norms[...] = norms[:, :ITERS] / total_cells
    rows = r0.shape[0]
    pieces = 2 if rows % 16 == 0 else 1
    size = rows // pieces
    copies = []
    for p in range(pieces):
        span = pl.ds(p * size, size)
        x[span] = y0 * fields[0, span] + y1 * fields[1, span] + y2 * fields[2, span]
        r[span] = (
            r0[span] - y0 * images[0, span] - y1 * images[1, span] - y2 * images[2, span]
        )
        for k, (src, dst) in enumerate(((x, out_x), (r, out_r))):
            copy = pltpu.make_async_copy(src.at[span], dst.at[span], sem.at[p, k])
            copy.start()
            copies.append(copy)
    for copy in copies:
        copy.wait()


def on_device(n_gx, n_gy, right_side, diagonal, horizontal, vertical, precond, edge_rows):
    rows, cols, levels = right_side.shape
    f32 = jnp.float32
    block = (rows * cols, levels)
    sems = pltpu.SemaphoreType.DMA
    basis = pltpu.VMEM((ITERS,) + block, f32)
    fields, images, totals, start = pl.pallas_call(
        functools.partial(kernel, n_gx, n_gy, rows),
        out_shape=(basis, basis, pltpu.VMEM((1, levels), f32), pltpu.VMEM(block, f32)),
        in_specs=[ANY, ANY, ANY, ANY, ANY, ANY],
        out_specs=(VMEM, VMEM, VMEM, VMEM),
        scratch_shapes=[
            pltpu.VMEM(block, f32),
            pltpu.VMEM(block, f32),
            pltpu.VMEM((1, levels), f32),
            pltpu.VMEM((levels, levels), f32),
            pltpu.VMEM((ITERS, 2 * rows, levels), f32),
            [pltpu.VMEM((n_gy * rows, levels), f32)] * ITERS,
            [pltpu.VMEM((n_gy * rows, levels), f32)] * ITERS,
            pltpu.VMEM((ITERS, cols, levels), f32),
            pltpu.VMEM((ITERS, cols, levels), f32),
            pltpu.VMEM((2 * rows, levels), f32),
            pltpu.VMEM((n_gx * n_gy, 1, levels), f32),
            pltpu.SMEM(edge_rows.shape, jnp.int32),
            sems((6,)),
            sems((ITERS, 2)),
            sems((ITERS,)),
            sems((ITERS,)),
            sems((ITERS, 2)),
            sems((ITERS,)),
            sems((ITERS,)),
            sems(()),
            sems(()),
        ],
        compiler_params=pltpu.CompilerParams(collective_id=0, has_side_effects=True),
    )(
        edge_rows,
        right_side.reshape(block),
        diagonal.reshape(block),
        horizontal.reshape(block),
        vertical.reshape(1, levels),
        precond,
    )
    in_vmem = functools.partial(
        pltpu.with_memory_space_constraint, memory_space=pltpu.VMEM
    )
    total_cells = float(rows * cols * levels * n_gx * n_gy)
    x, r, norms = pl.pallas_call(
        functools.partial(finish, total_cells),
        out_shape=(
            jax.ShapeDtypeStruct(block, f32),
            jax.ShapeDtypeStruct(block, f32),
            jax.ShapeDtypeStruct((1, ITERS), f32),
        ),
        in_specs=[VMEM, VMEM, VMEM, VMEM],
        out_specs=(ANY, ANY, VMEM),
        scratch_shapes=[pltpu.VMEM(block, f32), pltpu.VMEM(block, f32), sems((2, 2))],
    )(in_vmem(totals), in_vmem(start), in_vmem(fields), in_vmem(images))
    shape = right_side.shape
    return x.reshape(shape), r.reshape(shape), norms.reshape(ITERS)


def solution(mesh):
    n_gx, n_gy = mesh.shape["gx"], mesh.shape["gy"]
    field = P("gy", "gx", None)
    return jax.shard_map(
        functools.partial(on_device, n_gx, n_gy),
        mesh=mesh,
        in_specs=(field, field, field, P(), P(), P()),
        out_specs=(field, field, P()),
        check_vma=False,
    )
```
